32 devices in a mesh: rep: 4 (over x, core), grp: 8 (over z, y).
Axes of the slice: x: 2, y: 2, z: 4, core: 2. Of those that a mesh axis runs over, the one named last changes fastest.
Arguments:
- tokens: bfloat16 [8192, 2304], P(('rep', 'grp')), may hold values from -6 to 6
- norm_gain: float32 [2304], replicated, may hold values from 0.25 to 1.75
- key_weight: bfloat16 [2304, 1024], P('grp'), may hold values from -0.125 to 0.125
- key_grad: bfloat16 [8192, 1024], P(('rep', 'grp')), may hold values from -6 to 6
Outputs:
- token_grad: bfloat16 [8192, 2304], P(('rep', 'grp'))
- weight_grad: float32 [2304, 1024], P('grp', 'rep')
- gain_grad: float32 [2304], replicated
The draws below stay inside these ranges and needn't reach their ends.
All inputs are finite; a program needn't handle non-finite values.
Results may differ from the reference program's by a relative error of at most 0.023.
Values may be sent and summed in bfloat16 or wider, within the bound.
A program may use at most 64 MiB of HBM per device.

```python
import jax
import jax.numpy as jnp
from jax import lax

D = 2304
KV_HEADS = 8
HEAD_DIM = 128
KEYS = 1024
TOK_DEV = 256
TOKENS = 8192
N_REP = 4
N_GRP = 8


def block_levels(key, extent, pieces, low, largest):
    def one(axis_at, blocks):
        steps = jax.random.uniform(jax.random.fold_in(jax.random.fold_in(key, 6), axis_at), (blocks,), jnp.float32, low / len(pieces), largest / len(pieces))
        return jnp.repeat(jnp.exp(steps), extent[axis_at] // blocks).reshape((-1,) + (1,) * (len(extent) - axis_at - 1))

    loudness = one(*pieces[0])
    for cut in pieces[1:]:
        loudness = loudness * one(*cut)
    return loudness


def bell_draw(own_key, dims, spread, reach, shards=(), dtype=jnp.bfloat16):
    array = jax.random.normal(own_key, dims, jnp.float32) * spread
    if len(shards) > 0:
        array = block_levels(own_key, dims, shards, -0.22, 0.18) * array
    return jnp.clip(array, min=-reach, max=reach).astype(dtype)


def setup_inputs(seed: int = 0) -> dict:
    key_list = jax.random.split(jax.random.key(seed), 5)
    tokens = bell_draw(key_list[0], (TOKENS, D), 1.0, 6.0, ((0, 32),))
    norm_gain = jnp.clip(1.0 + 0.15 * jax.random.normal(key_list[1], (D,), jnp.float32), 0.25, 1.75)
    key_weight = bell_draw(key_list[2], (D, KEYS), D ** -0.5, 0.125, ((0, 8),))
    key_grad = bell_draw(key_list[3], (TOKENS, KEYS), 1.0, 6.0, ((0, 32),))
    return {"tokens": tokens, "norm_gain": norm_gain, "key_weight": key_weight, "key_grad": key_grad}


epsilon = 1e-06

def reference(tokens, norm_gain, key_weight, key_grad):
    grad_scale = (TOK_DEV * N_REP * N_GRP) ** (-0.5)
    blocks = tokens.reshape(N_REP * N_GRP, TOK_DEV, D)
    key_blocks = key_grad.reshape(N_REP * N_GRP, TOK_DEV, KV_HEADS * HEAD_DIM)

    def one_block(carry, inputs):
        running, gain_total = carry
        block_tokens, block_keys = inputs
        wide_tokens = block_tokens.astype(jnp.float32)
        inv_rms = lax.rsqrt(lax.optimization_barrier(jnp.mean(wide_tokens * wide_tokens, axis=1, keepdims=True)) + epsilon)
        normed = (wide_tokens * inv_rms * norm_gain).astype(jnp.bfloat16)
        partial_value = lax.dot_general(normed, block_keys, (((0,), (0,)), ((), ())), preferred_element_type=jnp.float32)
        rounded = lax.optimization_barrier(partial_value.astype(jnp.bfloat16)).astype(jnp.float32)
        d_normed = lax.dot_general(block_keys, key_weight, (((1,), (1,)), ((), ())), preferred_element_type=jnp.float32)
        gain_part = lax.optimization_barrier(jnp.sum(d_normed * wide_tokens * inv_rms, axis=0))
        scaled = d_normed * norm_gain
        inner_mean = lax.optimization_barrier(jnp.mean(scaled * wide_tokens, axis=1, keepdims=True))
        block_grad = (inv_rms * (scaled - wide_tokens * inv_rms * inv_rms * inner_mean)).astype(jnp.bfloat16)
        return ((running + rounded, gain_total + gain_part), block_grad)
    start = (jnp.zeros((D, KV_HEADS * HEAD_DIM), jnp.float32), jnp.zeros((D,), jnp.float32))
    (running, gain_total), grads = lax.scan(one_block, start, (blocks, key_blocks))
    token_grad = grads.reshape(N_REP * N_GRP * TOK_DEV, D)
    return (token_grad, running * grad_scale, gain_total * grad_scale)
```

```python
import functools

import jax
import jax.numpy as jnp
from jax import lax
from jax.experimental import pallas as pl
from jax.experimental.pallas import tpu as pltpu
from jax.sharding import PartitionSpec as P

epsilon = 1e-06
MESH = pl.DeviceIdType.MESH
LANES = 128


def flip(i, bits):
    bit = 1
    while bit <= bits:
        if bits & bit:
            i = i + bit * (1 - 2 * lax.rem(lax.div(i, bit), 2))
        bit *= 2
    return i


def kernel(
    n_z, grad_scale,
    tok_ref, gain_ref, w_ref, kg_ref,
    tg_ref, wg_ref, gg_ref,
    wfull, normed_t, dn, mine, give, take, in1, in2, in3, gsend, grecv,
    w_send, w_recv, c_send, c_recv, s1_send, s1_recv, s2_send, s2_recv, s3_send, s3_recv, g_send, g_recv,
):
    rep, grp = lax.axis_index("rep"), lax.axis_index("grp")
    x, c = lax.div(rep, 2), lax.rem(rep, 2)
    z, y = lax.div(grp, 2), lax.rem(grp, 2)
    rows, keys = w_ref.shape
    features = tok_ref.shape[1]
    cols = mine.shape[-1]
    peer_c = (2 * x + 1 - c, grp)
    peer_x = (2 * (1 - x) + c, grp)
    peer_y = (rep, 2 * z + 1 - y)
    peer_z = [None] + [(rep, 2 * flip(z, k) + y) for k in range(1, n_z)]

    barrier = pltpu.get_barrier_semaphore()
    peers = [peer_c, peer_x, peer_y] + peer_z[1:]
    for peer in peers:
        pl.semaphore_signal(barrier, inc=1, device_id=peer, device_id_type=MESH)
    pl.semaphore_wait(barrier, len(peers))

    sends = []

    def send(src, dst, s_sem, r_sem, peer):
        copy = pltpu.make_async_remote_copy(
            src_ref=src, dst_ref=dst, send_sem=s_sem, recv_sem=r_sem, device_id=peer, device_id_type=MESH
        )
        copy.start()
        sends.append(copy)

    def arrived(dst, sem):
        pltpu.make_async_remote_copy(
            src_ref=dst, dst_ref=dst, send_sem=sem, recv_sem=sem, device_id=peer_c, device_id_type=MESH
        ).wait_recv()

    def row_at(k, yy):
        g = 2 * flip(z, k) + (1 - y if yy else y)
        return pl.ds(pl.multiple_of(g * rows, 16), rows)

    def col_at(xx, cc):
        r = 2 * (1 - x if xx else x) + (1 - c if cc else c)
        return pl.ds(pl.multiple_of(r * cols, LANES), cols)

    def piece(xx, cc, k, yy):
        return wfull.at[row_at(k, yy), col_at(xx, cc)]

    def got(xx, cc, k, yy):
        arrived(piece(xx, cc, k, yy), w_recv.at[xx, cc, k, yy])

    def w_fwd(axis, xx, k, yy):
        there = {0: (xx, 1, k, yy), 1: (1 - xx, 0, k, yy), 2: (xx, 0, k, 1 - yy)}[axis]
        peer = (peer_c, peer_x, peer_y)[axis]
        ref = piece(xx, 0, k, yy)
        send(ref, ref, w_send.at[axis, xx, k, yy], w_recv.at[there], peer)

    own_cols = w_ref.at[:, col_at(0, 0)]
    for k in range(1, n_z):
        send(own_cols, piece(0, 0, 0, 0), w_send.at[3, 0, k, 0], w_recv.at[0, 0, k, 0], peer_z[k])
    send(own_cols, piece(0, 0, 0, 0), w_send.at[2, 0, 0, 0], w_recv.at[0, 0, 0, 1], peer_y)

    acc = None
    for j in range(features // LANES):
        t = tok_ref[:, j * LANES:(j + 1) * LANES].astype(jnp.float32)
        acc = t * t if acc is None else acc + t * t
    inv = lax.rsqrt(jnp.sum(acc, axis=1, keepdims=True) / features + epsilon)
    for j in range(features // LANES):
        at = slice(j * LANES, (j + 1) * LANES)
        t = tok_ref[:, at].astype(jnp.float32)
        normed_t[at, :] = (t * inv * gain_ref[:, at]).T.astype(jnp.bfloat16)

    def partial(k):
        for cc in (1, 0):
            for yy in (0, 1):
                for xx in (0, 1):
                    block = jnp.dot(
                        normed_t[row_at(k, yy), :], kg_ref[:, col_at(xx, cc)], preferred_element_type=jnp.float32
                    ).astype(jnp.bfloat16)
                    (give if cc else mine)[k, yy, xx] = block
            if cc:
                send(give.at[k], take.at[k], c_send.at[k], c_recv.at[k], peer_c)

    def add(k, yy, xx, ref):
        mine[k, yy, xx] = (
            mine[k, yy, xx].astype(jnp.float32) + ref[...].astype(jnp.float32)
        ).astype(jnp.bfloat16)

    def x_first(k):
        return k % 2 == 1

    def stage1(k):
        arrived(take.at[k], c_recv.at[k])
        order = [(0, 1), (1, 1), (0, 0), (1, 0)] if x_first(k) else [(1, 0), (1, 1), (0, 0), (0, 1)]
        for n, (yy, xx) in enumerate(order):
            add(k, yy, xx, take.at[k, yy, xx])
            if n < 2:
                slot = yy if x_first(k) else xx
                send(
                    mine.at[k, yy, xx], in1.at[k, slot], s1_send.at[k, slot], s1_recv.at[k, slot],
                    peer_x if x_first(k) else peer_y,
                )

    def stage2(k):
        for slot in (1, 0):
            arrived(in1.at[k, slot], s1_recv.at[k, slot])
            yy, xx = (slot, 0) if x_first(k) else (0, slot)
            add(k, yy, xx, in1.at[k, slot])
            if slot:
                send(mine.at[k, yy, xx], in2.at[k], s2_send.at[k], s2_recv.at[k], peer_y if x_first(k) else peer_x)

    def stage3(k):
        arrived(in2.at[k], s2_recv.at[k])
        add(k, 0, 0, in2.at[k])
        send(mine.at[k, 0, 0], in3.at[k], s3_send.at[k], s3_recv.at[k], peer_z[k])

    def from_z(k):
        got(0, 0, k, 0)
        for axis in (1, 2, 0):
            w_fwd(axis, 0, k, 0)

    def diag_by_x(k):
        return k == 0 or k == n_z - 1

    def from_x(k):
        got(1, 0, k, 0)
        if not diag_by_x(k):
            w_fwd(2, 1, k, 0)
        w_fwd(0, 1, k, 0)

    def from_y(k):
        got(0, 0, k, 1)
        if diag_by_x(k):
            w_fwd(1, 0, k, 1)
        w_fwd(0, 0, k, 1)

    wfull[row_at(0, 0), :] = w_ref[...]
    far = list(range(n_z - 1, -1, -1))
    near = list(range(1, n_z))
    partial(far[0])
    from_y(0)
    for n, k in enumerate(near):
        partial(far[n + 1])
        from_z(k)
        stage1(far[n])
    stage1(far[-1])
    for n, k in enumerate(near):
        from_x(k)
        from_y(k)
        stage2(far[n])
    stage2(far[-1])
    for k in range(n_z):
        got(1, 0, k, 1)
        w_fwd(0, 1, k, 1)
    for k in far[:-1]:
        stage3(k)
    for k in range(n_z):
        for yy in (0, 1):
            for xx in (0, 1):
                if k or yy:
                    got(xx, 1, k, yy)

    wide = 2 * LANES
    inner = jnp.zeros((tok_ref.shape[0], LANES), jnp.float32)
    for j in range(features // wide):
        at = slice(j * wide, (j + 1) * wide)
        d = lax.dot_general(
            kg_ref[...], wfull[at, :], (((1,), (1,)), ((), ())), preferred_element_type=jnp.float32
        )
        dn[:, at] = d
        dt = d * tok_ref[:, at].astype(jnp.float32)
        gsend[0, :, at] = jnp.sum(dt * inv, axis=0, keepdims=True)
        scaled = dt * gain_ref[:, at]
        inner = inner + scaled[:, :LANES] + scaled[:, LANES:]
    send(gsend.at[0], grecv.at[0], g_send.at[0], g_recv.at[0], peer_c)
    mean = jnp.sum(inner, axis=1, keepdims=True) / features
    pull = inv * inv * mean

    def token_grad(lo, hi):
        for j in range(lo, hi):
            at = slice(j * wide, (j + 1) * wide)
            t = tok_ref[:, at].astype(jnp.float32)
            tg_ref[:, at] = (inv * (dn[:, at] * gain_ref[:, at] - t * pull)).astype(jnp.bfloat16)

    steps = features // wide
    cuts = [steps * n // 3 for n in range(4)]
    for n, peer in enumerate((peer_x, peer_y, None)):
        token_grad(cuts[n], cuts[n + 1])
        arrived(grecv.at[n], g_recv.at[n])
        gsend[n + 1] = gsend[n] + grecv[n]
        if peer is not None:
            send(gsend.at[n + 1], grecv.at[n + 1], g_send.at[n + 1], g_recv.at[n + 1], peer)
        else:
            for k in range(1, n_z):
                send(gsend.at[n + 1], grecv.at[2 + k], g_send.at[2 + k], g_recv.at[2 + k], peer_z[k])

    arrived(in2.at[0], s2_recv.at[0])
    total = mine[0, 0, 0].astype(jnp.float32) + in2[0].astype(jnp.float32)
    for k in range(1, n_z):
        arrived(in3.at[k], s3_recv.at[k])
        total = total + in3[k].astype(jnp.float32)
    wg_ref[...] = total * grad_scale

    terms = [gsend[3]]
    for k in range(1, n_z):
        arrived(grecv.at[2 + k], g_recv.at[2 + k])
        terms.append(grecv[2 + k])
    while len(terms) > 1:
        terms = [terms[i] + terms[i + 1] for i in range(0, len(terms), 2)]
    gg_ref[...] = terms[0] * grad_scale
    for copy in sends:
        copy.wait_send()


def fused(n_rep, n_grp, tokens, norm_gain, key_weight, key_grad):
    n_tok, features = tokens.shape
    rows, keys = key_weight.shape
    cols, n_z = keys // n_rep, n_grp // 2
    grad_scale = (n_tok * n_rep * n_grp) ** (-0.5)
    vmem = pl.BlockSpec(memory_space=pltpu.VMEM)
    bf16, f32, dma = jnp.bfloat16, jnp.float32, pltpu.SemaphoreType.DMA
    block = (rows, cols)
    token_grad, weight_grad, gain_grad = pl.pallas_call(
        functools.partial(kernel, n_z, grad_scale),
        out_shape=(
            jax.ShapeDtypeStruct((n_tok, features), bf16),
            jax.ShapeDtypeStruct(block, f32),
            jax.ShapeDtypeStruct((1, features), f32),
        ),
        in_specs=[vmem] * 4,
        out_specs=(vmem,) * 3,
        scratch_shapes=[
            pltpu.VMEM((features, keys), bf16),
            pltpu.VMEM((features, n_tok), bf16),
            pltpu.VMEM((n_tok, features), f32),
            pltpu.VMEM((n_z, 2, 2) + block, bf16),
            pltpu.VMEM((n_z, 2, 2) + block, bf16),
            pltpu.VMEM((n_z, 2, 2) + block, bf16),
            pltpu.VMEM((n_z, 2) + block, bf16),
            pltpu.VMEM((n_z,) + block, bf16),
            pltpu.VMEM((n_z,) + block, bf16),
            pltpu.VMEM((4, 1, features), f32),
            pltpu.VMEM((n_z + 2, 1, features), f32),
            dma((4, 2, n_z, 2)), dma((2, 2, n_z, 2)),
            dma((n_z,)), dma((n_z,)),
            dma((n_z, 2)), dma((n_z, 2)),
            dma((n_z,)), dma((n_z,)),
            dma((n_z,)), dma((n_z,)),
            dma((n_z + 2,)), dma((n_z + 2,)),
        ],
        compiler_params=pltpu.CompilerParams(
            collective_id=0, has_side_effects=True, vmem_limit_bytes=48 * 1024 * 1024
        ),
    )(tokens, norm_gain.reshape(1, features), key_weight, key_grad)
    return token_grad, weight_grad, gain_grad.reshape(features)


def plain(tokens, norm_gain, key_weight, key_grad):
    total_tokens = tokens.shape[0] * lax.axis_size("rep") * lax.axis_size("grp")
    grad_scale = total_tokens ** (-0.5)
    wide_tokens = tokens.astype(jnp.float32)
    inv_rms = lax.rsqrt(jnp.mean(wide_tokens * wide_tokens, axis=1, keepdims=True) + epsilon)
    normed = (wide_tokens * inv_rms * norm_gain).astype(jnp.bfloat16)
    partial_value = lax.dot_general(
        normed, key_grad, (((0,), (0,)), ((), ())), preferred_element_type=jnp.float32
    )
    d_normed = lax.dot_general(
        key_grad,
        lax.all_gather(key_weight, "grp", axis=0, tiled=True),
        (((1,), (1,)), ((), ())),
        preferred_element_type=jnp.float32,
    )
    section_one = lax.psum_scatter(
        partial_value.astype(jnp.bfloat16), "rep", scatter_dimension=1, tiled=True
    ).astype(jnp.float32)
    weight_sum = lax.psum_scatter(section_one, "grp", scatter_dimension=0, tiled=True)
    gain_local = jnp.sum(d_normed * wide_tokens * inv_rms, axis=0)
    gain_total = lax.psum(gain_local, ("rep", "grp"))
    scaled = d_normed * norm_gain
    inner_mean = jnp.mean(scaled * wide_tokens, axis=1, keepdims=True)
    token_grad = (inv_rms * (scaled - wide_tokens * inv_rms * inv_rms * inner_mean)).astype(
        jnp.bfloat16
    )
    return (token_grad, weight_sum * grad_scale, gain_total * grad_scale)


def shards(tokens, norm_gain, key_weight, key_grad):
    n_rep, n_grp = lax.axis_size("rep"), lax.axis_size("grp")
    n_z = n_grp // 2
    if (
        n_rep == 2 * 2 and n_grp % 2 == 0 and n_z & (n_z - 1) == 0 and 1 < n_z <= 4
        and key_weight.shape[1] % (n_rep * LANES) == 0 and key_weight.shape[0] % 16 == 0
        and tokens.shape[1] % (2 * LANES) == 0 and tokens.shape[0] % LANES == 0
    ):
        return fused(n_rep, n_grp, tokens, norm_gain, key_weight, key_grad)
    return plain(tokens, norm_gain, key_weight, key_grad)


def solution(mesh):
    in_specs = (P(("rep", "grp"), None), P(), P("grp", None), P(("rep", "grp"), None))
    out_specs = (P(("rep", "grp"), None), P("grp", "rep"), P())
    return jax.shard_map(shards, mesh=mesh, in_specs=in_specs, out_specs=out_specs, check_vma=False)
```

```python
import functools

import jax
import jax.numpy as jnp
from jax import lax
from jax.experimental import pallas as pl
from jax.experimental.pallas import tpu as pltpu
from jax.sharding import PartitionSpec as P

epsilon = 1e-06
MESH = pl.DeviceIdType.MESH
LANES = 128


def flip(i, bits):
    bit = 1
    while bit <= bits:
        if bits & bit:
            i = i + bit * (1 - 2 * lax.rem(lax.div(i, bit), 2))
        bit *= 2
    return i


def kernel(
    n_z, grad_scale,
    tok_hbm, gain_hbm, w_ref, kg_hbm,
    tg_ref, wg_ref, gg_ref,
    tok_ref, gain_ref, kg_ref, load_sem, wfull, normed_t, dn, mine, give, take, in1, in2, in3, gsend, grecv,
    w_send, w_recv, c_send, c_recv, s1_send, s1_recv, s2_send, s2_recv, s3_send, s3_recv, g_send, g_recv,
):
    rep, grp = lax.axis_index("rep"), lax.axis_index("grp")
    x, c = lax.div(rep, 2), lax.rem(rep, 2)
    z, y = lax.div(grp, 2), lax.rem(grp, 2)
    rows, keys = w_ref.shape
    features = tok_ref.shape[1]
    cols = mine.shape[-1]
    peer_c = (2 * x + 1 - c, grp)
    peer_x = (2 * (1 - x) + c, grp)
    peer_y = (rep, 2 * z + 1 - y)
    peer_z = [None] + [(rep, 2 * flip(z, k) + y) for k in range(1, n_z)]

    def row_at(k, yy):
        g = 2 * flip(z, k) + (1 - y if yy else y)
        return pl.ds(pl.multiple_of(g * rows, 16), rows)

    loads = [
        pltpu.make_async_copy(src, dst, load_sem.at[n])
        for n, (src, dst) in enumerate(
            ((tok_hbm, tok_ref), (gain_hbm, gain_ref), (kg_hbm, kg_ref), (w_ref, wfull.at[row_at(0, 0), :]))
        )
    ]
    for load in loads:
        load.start()

    barrier = pltpu.get_barrier_semaphore()
    peers = [peer_c, peer_x, peer_y] + peer_z[1:]
    for peer in peers:
        pl.semaphore_signal(barrier, inc=1, device_id=peer, device_id_type=MESH)
    pl.semaphore_wait(barrier, len(peers))

    sends = []

    def send(src, dst, s_sem, r_sem, peer):
        copy = pltpu.make_async_remote_copy(
            src_ref=src, dst_ref=dst, send_sem=s_sem, recv_sem=r_sem, device_id=peer, device_id_type=MESH
        )
        copy.start()
        sends.append(copy)

    def arrived(dst, sem):
        pltpu.make_async_remote_copy(
            src_ref=dst, dst_ref=dst, send_sem=sem, recv_sem=sem, device_id=peer_c, device_id_type=MESH
        ).wait_recv()

    def col_at(xx, cc):
        r = 2 * (1 - x if xx else x) + (1 - c if cc else c)
        return pl.ds(pl.multiple_of(r * cols, LANES), cols)

    def piece(xx, cc, k, yy):
        return wfull.at[row_at(k, yy), col_at(xx, cc)]

    def got(xx, cc, k, yy):
        arrived(piece(xx, cc, k, yy), w_recv.at[xx, cc, k, yy])

    def w_fwd(axis, xx, k, yy):
        there = {0: (xx, 1, k, yy), 1: (1 - xx, 0, k, yy), 2: (xx, 0, k, 1 - yy)}[axis]
        peer = (peer_c, peer_x, peer_y)[axis]
        ref = piece(xx, 0, k, yy)
        send(ref, ref, w_send.at[axis, xx, k, yy], w_recv.at[there], peer)

    def own_to(axis, xx, k, peer):
        there = (xx, 0, 0, 1) if axis == 2 else (xx, 0, k, 0)
        send(
            w_ref.at[:, col_at(xx, 0)], piece(xx, 0, 0, 0), w_send.at[axis, xx, k, 0], w_recv.at[there], peer
        )

    own_to(2, 0, 0, peer_y)
    for k in range(1, n_z):
        own_to(3, 0, k, peer_z[k])
    own_to(2, 1, 0, peer_y)
    for k in range(1, n_z - 1):
        own_to(3, 1, k, peer_z[k])

    loads[0].wait()
    acc = None
    for j in range(features // LANES):
        t = tok_ref[:, j * LANES:(j + 1) * LANES].astype(jnp.float32)
        acc = t * t if acc is None else acc + t * t
    inv = lax.rsqrt(jnp.sum(acc, axis=1, keepdims=True) / features + epsilon)
    loads[1].wait()
    for j in range(features // LANES):
        at = slice(j * LANES, (j + 1) * LANES)
        t = tok_ref[:, at].astype(jnp.float32)
        normed_t[at, :] = (t * inv * gain_ref[at].reshape(1, -1)).T.astype(jnp.bfloat16)

    def partial(k):
        for cc in (1, 0):
            for yy in (0, 1):
                for xx in (0, 1):
                    block = jnp.dot(
                        normed_t[row_at(k, yy), :], kg_ref[:, col_at(xx, cc)], preferred_element_type=jnp.float32
                    ).astype(jnp.bfloat16)
                    (give if cc else mine)[k, yy, xx] = block
            if cc:
                send(give.at[k], take.at[k], c_send.at[k], c_recv.at[k], peer_c)

    def add(k, yy, xx, ref):
        mine[k, yy, xx] = (
            mine[k, yy, xx].astype(jnp.float32) + ref[...].astype(jnp.float32)
        ).astype(jnp.bfloat16)

    def x_first(k):
        return k % 2 == 1

    def core_in(k):
        arrived(take.at[k], c_recv.at[k])

    def stage1(k, slot):
        for other in (1, 0):
            yy, xx = (slot, other) if x_first(k) else (other, slot)
            add(k, yy, xx, take.at[k, yy, xx])
            if other:
                send(
                    mine.at[k, yy, xx], in1.at[k, slot], s1_send.at[k, slot], s1_recv.at[k, slot],
                    peer_x if x_first(k) else peer_y,
                )

    def stage2(k, slot):
        arrived(in1.at[k, slot], s1_recv.at[k, slot])
        yy, xx = (slot, 0) if x_first(k) else (0, slot)
        add(k, yy, xx, in1.at[k, slot])
        if slot:
            send(mine.at[k, yy, xx], in2.at[k], s2_send.at[k], s2_recv.at[k], peer_y if x_first(k) else peer_x)

    def stage3(k):
        arrived(in2.at[k], s2_recv.at[k])
        add(k, 0, 0, in2.at[k])
        send(mine.at[k, 0, 0], in3.at[k], s3_send.at[k], s3_recv.at[k], peer_z[k])

    def take_on(xx, k, yy, *axes):
        got(xx, 0, k, yy)
        for axis in axes + (0,):
            w_fwd(axis, xx, k, yy)

    loads[2].wait()
    partial(3)
    take_on(0, 1, 0, 2)
    partial(2)
    core_in(3)
    stage1(3, 1)
    stage1(3, 0)
    take_on(0, 2, 0, 2)
    core_in(2)
    stage1(2, 1)
    stage1(2, 0)
    take_on(0, 0, 1)
    take_on(0, 1, 1, 1)
    partial(1)
    partial(0)
    take_on(0, 2, 1, 1)
    stage2(3, 1)
    take_on(0, 3, 0, 1, 2)
    core_in(1)
    core_in(0)
    stage2(3, 0)
    take_on(1, 0, 1)
    take_on(1, 1, 0)
    stage2(2, 1)
    take_on(1, 1, 1)
    stage1(1, 1)
    stage1(0, 1)
    stage1(0, 0)
    take_on(1, 2, 1)
    take_on(0, 3, 1, 1)
    stage1(1, 0)
    take_on(1, 2, 0)
    stage2(2, 0)
    take_on(1, 3, 0)
    stage3(3)
    stage3(2)
    stage2(1, 1)
    stage2(0, 1)
    take_on(1, 3, 1)
    loads[3].wait()
    for k in range(n_z):
        for yy in (0, 1):
            for xx in (0, 1):
                if k or yy:
                    got(xx, 1, k, yy)

    wide = 2 * LANES
    inner = jnp.zeros((tok_ref.shape[0], LANES), jnp.float32)
    for j in range(features // wide):
        at = slice(j * wide, (j + 1) * wide)
        d = lax.dot_general(
            kg_ref[...], wfull[at, :], (((1,), (1,)), ((), ())), preferred_element_type=jnp.float32
        )
        dn[:, at] = d
        dt = d * tok_ref[:, at].astype(jnp.float32)
        gsend[0, :, at] = jnp.sum(dt * inv, axis=0, keepdims=True)
        scaled = dt * gain_ref[at].reshape(1, -1)
        inner = inner + scaled[:, :LANES] + scaled[:, LANES:]
    send(gsend.at[0], grecv.at[0], g_send.at[0], g_recv.at[0], peer_c)
    for k in (1, 0):
        stage2(k, 0)
    stage3(1)
    mean = jnp.sum(inner, axis=1, keepdims=True) / features
    pull = inv * inv * mean

    def token_grad(lo, hi):
        for j in range(lo, hi):
            at = slice(j * wide, (j + 1) * wide)
            t = tok_ref[:, at].astype(jnp.float32)
            tg_ref[:, at] = (inv * (dn[:, at] * gain_ref[at].reshape(1, -1) - t * pull)).astype(jnp.bfloat16)

    steps = features // wide
    cuts = [steps * n // 3 for n in range(4)]
    for n, peer in enumerate((peer_x, peer_y, None)):
        token_grad(cuts[n], cuts[n + 1])
        arrived(grecv.at[n], g_recv.at[n])
        gsend[n + 1] = gsend[n] + grecv[n]
        if peer is not None:
            send(gsend.at[n + 1], grecv.at[n + 1], g_send.at[n + 1], g_recv.at[n + 1], peer)
        else:
            for k in range(1, n_z):
                send(gsend.at[n + 1], grecv.at[2 + k], g_send.at[2 + k], g_recv.at[2 + k], peer_z[k])

    arrived(in2.at[0], s2_recv.at[0])
    total = mine[0, 0, 0].astype(jnp.float32) + in2[0].astype(jnp.float32)
    for k in range(1, n_z):
        arrived(in3.at[k], s3_recv.at[k])
        total = total + in3[k].astype(jnp.float32)
    wg_ref[...] = total * grad_scale

    terms = [gsend[3]]
    for k in range(1, n_z):
        arrived(grecv.at[2 + k], g_recv.at[2 + k])
        terms.append(grecv[2 + k])
    while len(terms) > 1:
        terms = [terms[i] + terms[i + 1] for i in range(0, len(terms), 2)]
    total = terms[0] * grad_scale
    for j in range(features // LANES):
        at = slice(j * LANES, (j + 1) * LANES)
        gg_ref[at] = total[:, at].reshape(LANES)
    for copy in sends:
        copy.wait_send()


def fused(n_rep, n_grp, tokens, norm_gain, key_weight, key_grad):
    n_tok, features = tokens.shape
    rows, keys = key_weight.shape
    cols, n_z = keys // n_rep, n_grp // 2
    grad_scale = (n_tok * n_rep * n_grp) ** (-0.5)
    vmem = pl.BlockSpec(memory_space=pltpu.VMEM)
    bf16, f32, dma = jnp.bfloat16, jnp.float32, pltpu.SemaphoreType.DMA
    block = (rows, cols)
    token_grad, weight_grad, gain_grad = pl.pallas_call(
        functools.partial(kernel, n_z, grad_scale),
        out_shape=(
            jax.ShapeDtypeStruct((n_tok, features), bf16),
            jax.ShapeDtypeStruct(block, f32),
            jax.ShapeDtypeStruct((features,), f32),
        ),
        in_specs=[pl.BlockSpec(memory_space=pl.ANY)] * 4,
        out_specs=(vmem,) * 3,
        scratch_shapes=[
            pltpu.VMEM((n_tok, features), bf16),
            pltpu.VMEM((features,), f32),
            pltpu.VMEM((n_tok, keys), bf16),
            dma((4,)),
            pltpu.VMEM((features, keys), bf16),
            pltpu.VMEM((features, n_tok), bf16),
            pltpu.VMEM((n_tok, features), f32),
            pltpu.VMEM((n_z, 2, 2) + block, bf16),
            pltpu.VMEM((n_z, 2, 2) + block, bf16),
            pltpu.VMEM((n_z, 2, 2) + block, bf16),
            pltpu.VMEM((n_z, 2) + block, bf16),
            pltpu.VMEM((n_z,) + block, bf16),
            pltpu.VMEM((n_z,) + block, bf16),
            pltpu.VMEM((4, 1, features), f32),
            pltpu.VMEM((n_z + 2, 1, features), f32),
            dma((4, 2, n_z, 2)), dma((2, 2, n_z, 2)),
            dma((n_z,)), dma((n_z,)),
            dma((n_z, 2)), dma((n_z, 2)),
            dma((n_z,)), dma((n_z,)),
            dma((n_z,)), dma((n_z,)),
            dma((n_z + 2,)), dma((n_z + 2,)),
        ],
        compiler_params=pltpu.CompilerParams(
            collective_id=0, has_side_effects=True, vmem_limit_bytes=60 * 1024 * 1024
        ),
    )(tokens, norm_gain, key_weight, key_grad)
    return token_grad, weight_grad, gain_grad


def plain(tokens, norm_gain, key_weight, key_grad):
    total_tokens = tokens.shape[0] * lax.axis_size("rep") * lax.axis_size("grp")
    grad_scale = total_tokens ** (-0.5)
    wide_tokens = tokens.astype(jnp.float32)
    inv_rms = lax.rsqrt(jnp.mean(wide_tokens * wide_tokens, axis=1, keepdims=True) + epsilon)
    normed = (wide_tokens * inv_rms * norm_gain).astype(jnp.bfloat16)
    partial_value = lax.dot_general(
        normed, key_grad, (((0,), (0,)), ((), ())), preferred_element_type=jnp.float32
    )
    d_normed = lax.dot_general(
        key_grad,
        lax.all_gather(key_weight, "grp", axis=0, tiled=True),
        (((1,), (1,)), ((), ())),
        preferred_element_type=jnp.float32,
    )
    section_one = lax.psum_scatter(
        partial_value.astype(jnp.bfloat16), "rep", scatter_dimension=1, tiled=True
    ).astype(jnp.float32)
    weight_sum = lax.psum_scatter(section_one, "grp", scatter_dimension=0, tiled=True)
    gain_local = jnp.sum(d_normed * wide_tokens * inv_rms, axis=0)
    gain_total = lax.psum(gain_local, ("rep", "grp"))
    scaled = d_normed * norm_gain
    inner_mean = jnp.mean(scaled * wide_tokens, axis=1, keepdims=True)
    token_grad = (inv_rms * (scaled - wide_tokens * inv_rms * inv_rms * inner_mean)).astype(
        jnp.bfloat16
    )
    return (token_grad, weight_sum * grad_scale, gain_total * grad_scale)


def shards(tokens, norm_gain, key_weight, key_grad):
    n_rep, n_grp = lax.axis_size("rep"), lax.axis_size("grp")
    n_z = n_grp // 2
    if (
        n_rep == 2 * 2 and n_grp == 2 * 4
        and key_weight.shape[1] % (n_rep * LANES) == 0 and key_weight.shape[0] % 16 == 0
        and tokens.shape[1] % (2 * LANES) == 0 and tokens.shape[0] % LANES == 0
    ):
        return fused(n_rep, n_grp, tokens, norm_gain, key_weight, key_grad)
    return plain(tokens, norm_gain, key_weight, key_grad)


def solution(mesh):
    in_specs = (P(("rep", "grp"), None), P(), P("grp", None), P(("rep", "grp"), None))
    out_specs = (P(("rep", "grp"), None), P("grp", "rep"), P())
    return jax.shard_map(shards, mesh=mesh, in_specs=in_specs, out_specs=out_specs, check_vma=False)
```

```python
import functools

import jax
import jax.numpy as jnp
from jax import lax
from jax.experimental import pallas as pl
from jax.experimental.pallas import tpu as pltpu
from jax.sharding import PartitionSpec as P

epsilon = 1e-06
MESH = pl.DeviceIdType.MESH
LANES = 128


def flip(i, bits):
    bit = 1
    while bit <= bits:
        if bits & bit:
            i = i + bit * (1 - 2 * lax.rem(lax.div(i, bit), 2))
        bit *= 2
    return i


def kernel(
    n_z, grad_scale,
    tok_hbm, gain_hbm, w_ref, kg_hbm,
    tg_ref, wg_ref, gg_ref,
    tok_ref, gain_ref, kg_ref, load_sem, wfull, normed_t, dn, mine, give, take, in1, in2, in3, gsend, grecv,
    w_send, w_recv, c_send, c_recv, s1_send, s1_recv, s2_send, s2_recv, s3_send, s3_recv, g_send, g_recv,
):
    rep, grp = lax.axis_index("rep"), lax.axis_index("grp")
    x, c = lax.div(rep, 2), lax.rem(rep, 2)
    z, y = lax.div(grp, 2), lax.rem(grp, 2)
    rows, keys = w_ref.shape
    features = tok_ref.shape[1]
    cols = mine.shape[-1]
    peer_c = (2 * x + 1 - c, grp)
    peer_x = (2 * (1 - x) + c, grp)
    peer_cx = (2 * (1 - x) + 1 - c, grp)
    peer_y = (rep, 2 * z + 1 - y)
    peer_z = [None] + [(rep, 2 * flip(z, k) + y) for k in range(1, n_z)]
    group = [peer_y]
    for k in range(1, n_z):
        group += [peer_z[k], (rep, 2 * flip(z, k) + 1 - y)]

    def row_at(k, yy):
        g = 2 * flip(z, k) + (1 - y if yy else y)
        return pl.ds(pl.multiple_of(g * rows, 16), rows)

    loads = [
        pltpu.make_async_copy(src, dst, load_sem.at[n])
        for n, (src, dst) in enumerate(
            ((tok_hbm, tok_ref), (gain_hbm, gain_ref), (kg_hbm, kg_ref), (w_ref, wfull.at[row_at(0, 0), :]))
        )
    ]
    for load in loads:
        load.start()

    barrier = pltpu.get_barrier_semaphore()
    peers = [peer_c, peer_x, peer_cx] + group
    for peer in peers:
        pl.semaphore_signal(barrier, inc=1, device_id=peer, device_id_type=MESH)
    pl.semaphore_wait(barrier, len(peers))

    sends = []

    def send(src, dst, s_sem, r_sem, peer):
        copy = pltpu.make_async_remote_copy(
            src_ref=src, dst_ref=dst, send_sem=s_sem, recv_sem=r_sem, device_id=peer, device_id_type=MESH
        )
        copy.start()
        sends.append(copy)

    def arrived(dst, sem):
        pltpu.make_async_remote_copy(
            src_ref=dst, dst_ref=dst, send_sem=sem, recv_sem=sem, device_id=peer_c, device_id_type=MESH
        ).wait_recv()

    def col_at(xx, cc):
        r = 2 * (1 - x if xx else x) + (1 - c if cc else c)
        return pl.ds(pl.multiple_of(r * cols, LANES), cols)

    def piece(xx, cc, k, yy):
        return wfull.at[row_at(k, yy), col_at(xx, cc)]

    def got(xx, cc, k, yy):
        arrived(piece(xx, cc, k, yy), w_recv.at[xx, cc, k, yy])

    def w_fwd(axis, xx, k, yy):
        there = {0: (xx, 1, k, yy), 1: (1 - xx, 0, k, yy), 2: (xx, 0, k, 1 - yy)}[axis]
        peer = (peer_c, peer_x, peer_y)[axis]
        ref = piece(xx, 0, k, yy)
        send(ref, ref, w_send.at[axis, xx, k, yy], w_recv.at[there], peer)

    def own_to(axis, xx, k, peer):
        there = (xx, 0, 0, 1) if axis == 2 else (xx, 0, k, 0)
        send(
            w_ref.at[:, col_at(xx, 0)], piece(xx, 0, 0, 0), w_send.at[axis, xx, k, 0], w_recv.at[there], peer
        )

    own_to(2, 0, 0, peer_y)
    for k in range(1, n_z):
        own_to(3, 0, k, peer_z[k])
    own_to(2, 1, 0, peer_y)
    for k in range(1, n_z - 1):
        own_to(3, 1, k, peer_z[k])

    loads[0].wait()
    acc = None
    for j in range(features // LANES):
        t = tok_ref[:, j * LANES:(j + 1) * LANES].astype(jnp.float32)
        acc = t * t if acc is None else acc + t * t
    inv = lax.rsqrt(jnp.sum(acc, axis=1, keepdims=True) / features + epsilon)
    loads[1].wait()
    for j in range(features // LANES):
        at = slice(j * LANES, (j + 1) * LANES)
        t = tok_ref[:, at].astype(jnp.float32)
        normed_t[at, :] = (t * inv * gain_ref[at].reshape(1, -1)).T.astype(jnp.bfloat16)

    def partial(k):
        for cc in (1, 0):
            for yy in (0, 1):
                for xx in (0, 1):
                    block = jnp.dot(
                        normed_t[row_at(k, yy), :], kg_ref[:, col_at(xx, cc)], preferred_element_type=jnp.float32
                    ).astype(jnp.bfloat16)
                    (give if cc else mine)[k, yy, xx] = block
            if cc:
                send(give.at[k], take.at[k], c_send.at[k], c_recv.at[k], peer_c)

    def add(k, yy, xx, ref):
        mine[k, yy, xx] = (
            mine[k, yy, xx].astype(jnp.float32) + ref[...].astype(jnp.float32)
        ).astype(jnp.bfloat16)

    def x_first(k):
        return k % 2 == 1

    def core_in(k):
        arrived(take.at[k], c_recv.at[k])

    def stage1(k, slot):
        for other in (1, 0):
            yy, xx = (slot, other) if x_first(k) else (other, slot)
            add(k, yy, xx, take.at[k, yy, xx])
            if other:
                send(
                    mine.at[k, yy, xx], in1.at[k, slot], s1_send.at[k, slot], s1_recv.at[k, slot],
                    peer_x if x_first(k) else peer_y,
                )

    def stage2(k, slot):
        arrived(in1.at[k, slot], s1_recv.at[k, slot])
        yy, xx = (slot, 0) if x_first(k) else (0, slot)
        add(k, yy, xx, in1.at[k, slot])
        if slot:
            send(mine.at[k, yy, xx], in2.at[k], s2_send.at[k], s2_recv.at[k], peer_y if x_first(k) else peer_x)

    def stage3(k):
        arrived(in2.at[k], s2_recv.at[k])
        add(k, 0, 0, in2.at[k])
        send(mine.at[k, 0, 0], in3.at[k], s3_send.at[k], s3_recv.at[k], peer_z[k])

    def take_on(xx, k, yy, *axes):
        got(xx, 0, k, yy)
        for axis in axes + (0,):
            w_fwd(axis, xx, k, yy)

    loads[2].wait()
    partial(3)
    take_on(0, 1, 0, 2)
    partial(2)
    core_in(3)
    stage1(3, 1)
    stage1(3, 0)
    take_on(0, 2, 0, 2)
    core_in(2)
    stage1(2, 1)
    stage1(2, 0)
    take_on(0, 0, 1)
    take_on(0, 1, 1, 1)
    partial(1)
    partial(0)
    take_on(0, 2, 1, 1)
    stage2(3, 1)
    take_on(0, 3, 0, 1, 2)
    core_in(1)
    core_in(0)
    stage2(3, 0)
    take_on(1, 0, 1)
    take_on(1, 1, 0)
    stage2(2, 1)
    take_on(1, 1, 1)
    stage1(1, 1)
    stage1(0, 1)
    stage1(0, 0)
    take_on(1, 2, 1)
    take_on(0, 3, 1, 1)
    stage1(1, 0)
    take_on(1, 2, 0)
    stage2(2, 0)
    take_on(1, 3, 0)
    stage3(3)
    stage3(2)
    stage2(1, 1)
    stage2(0, 1)
    take_on(1, 3, 1)
    loads[3].wait()
    for k in range(n_z):
        for yy in (0, 1):
            for xx in (0, 1):
                if k or yy:
                    got(xx, 1, k, yy)

    wide = 2 * LANES
    inner = jnp.zeros((tok_ref.shape[0], LANES), jnp.float32)
    for j in range(features // wide):
        at = slice(j * wide, (j + 1) * wide)
        d = lax.dot_general(
            kg_ref[...], wfull[at, :], (((1,), (1,)), ((), ())), preferred_element_type=jnp.float32
        )
        dn[:, at] = d
        dt = d * tok_ref[:, at].astype(jnp.float32)
        gsend[0, :, at] = jnp.sum(dt * inv, axis=0, keepdims=True)
        scaled = dt * gain_ref[at].reshape(1, -1)
        inner = inner + scaled[:, :LANES] + scaled[:, LANES:]
    for n, peer in enumerate((peer_c, peer_x, peer_cx)):
        send(gsend.at[0], grecv.at[n], g_send.at[n], g_recv.at[n], peer)
    for k in (1, 0):
        stage2(k, 0)
    stage3(1)
    mean = jnp.sum(inner, axis=1, keepdims=True) / features
    pull = inv * inv * mean

    def token_grad(lo, hi):
        for j in range(lo, hi):
            at = slice(j * wide, (j + 1) * wide)
            t = tok_ref[:, at].astype(jnp.float32)
            tg_ref[:, at] = (inv * (dn[:, at] * gain_ref[at].reshape(1, -1) - t * pull)).astype(jnp.bfloat16)

    steps = features // wide
    token_grad(0, steps // 3)
    for n in range(3):
        arrived(grecv.at[n], g_recv.at[n])
    gsend[1] = (gsend[0] + grecv[0]) + (grecv[1] + grecv[2])
    for n, peer in enumerate(group):
        send(gsend.at[1], grecv.at[3 + n], g_send.at[3 + n], g_recv.at[3 + n], peer)
    token_grad(steps // 3, steps)

    arrived(in2.at[0], s2_recv.at[0])
    total = mine[0, 0, 0].astype(jnp.float32) + in2[0].astype(jnp.float32)
    for k in range(1, n_z):
        arrived(in3.at[k], s3_recv.at[k])
        total = total + in3[k].astype(jnp.float32)
    wg_ref[...] = total * grad_scale

    terms = [gsend[1]]
    for n in range(3, 3 + len(group)):
        arrived(grecv.at[n], g_recv.at[n])
        terms.append(grecv[n])
    while len(terms) > 1:
        terms = [terms[i] + terms[i + 1] for i in range(0, len(terms), 2)]
    total = terms[0] * grad_scale
    for j in range(features // LANES):
        at = slice(j * LANES, (j + 1) * LANES)
        gg_ref[at] = total[:, at].reshape(LANES)
    for copy in sends:
        copy.wait_send()


def fused(n_rep, n_grp, tokens, norm_gain, key_weight, key_grad):
    n_tok, features = tokens.shape
    rows, keys = key_weight.shape
    cols, n_z = keys // n_rep, n_grp // 2
    grad_scale = (n_tok * n_rep * n_grp) ** (-0.5)
    vmem = pl.BlockSpec(memory_space=pltpu.VMEM)
    bf16, f32, dma = jnp.bfloat16, jnp.float32, pltpu.SemaphoreType.DMA
    block = (rows, cols)
    token_grad, weight_grad, gain_grad = pl.pallas_call(
        functools.partial(kernel, n_z, grad_scale),
        out_shape=(
            jax.ShapeDtypeStruct((n_tok, features), bf16),
            jax.ShapeDtypeStruct(block, f32),
            jax.ShapeDtypeStruct((features,), f32),
        ),
        in_specs=[pl.BlockSpec(memory_space=pl.ANY)] * 4,
        out_specs=(vmem,) * 3,
        scratch_shapes=[
            pltpu.VMEM((n_tok, features), bf16),
            pltpu.VMEM((features,), f32),
            pltpu.VMEM((n_tok, keys), bf16),
            dma((4,)),
            pltpu.VMEM((features, keys), bf16),
            pltpu.VMEM((features, n_tok), bf16),
            pltpu.VMEM((n_tok, features), f32),
            pltpu.VMEM((n_z, 2, 2) + block, bf16),
            pltpu.VMEM((n_z, 2, 2) + block, bf16),
            pltpu.VMEM((n_z, 2, 2) + block, bf16),
            pltpu.VMEM((n_z, 2) + block, bf16),
            pltpu.VMEM((n_z,) + block, bf16),
            pltpu.VMEM((n_z,) + block, bf16),
            pltpu.VMEM((2, 1, features), f32),
            pltpu.VMEM((2 * n_z + 2, 1, features), f32),
            dma((4, 2, n_z, 2)), dma((2, 2, n_z, 2)),
            dma((n_z,)), dma((n_z,)),
            dma((n_z, 2)), dma((n_z, 2)),
            dma((n_z,)), dma((n_z,)),
            dma((n_z,)), dma((n_z,)),
            dma((2 * n_z + 2,)), dma((2 * n_z + 2,)),
        ],
        compiler_params=pltpu.CompilerParams(
            collective_id=0, has_side_effects=True, vmem_limit_bytes=60 * 1024 * 1024
        ),
    )(tokens, norm_gain, key_weight, key_grad)
    return token_grad, weight_grad, gain_grad


def plain(tokens, norm_gain, key_weight, key_grad):
    total_tokens = tokens.shape[0] * lax.axis_size("rep") * lax.axis_size("grp")
    grad_scale = total_tokens ** (-0.5)
    wide_tokens = tokens.astype(jnp.float32)
    inv_rms = lax.rsqrt(jnp.mean(wide_tokens * wide_tokens, axis=1, keepdims=True) + epsilon)
    normed = (wide_tokens * inv_rms * norm_gain).astype(jnp.bfloat16)
    partial_value = lax.dot_general(
        normed, key_grad, (((0,), (0,)), ((), ())), preferred_element_type=jnp.float32
    )
    d_normed = lax.dot_general(
        key_grad,
        lax.all_gather(key_weight, "grp", axis=0, tiled=True),
        (((1,), (1,)), ((), ())),
        preferred_element_type=jnp.float32,
    )
    section_one = lax.psum_scatter(
        partial_value.astype(jnp.bfloat16), "rep", scatter_dimension=1, tiled=True
    ).astype(jnp.float32)
    weight_sum = lax.psum_scatter(section_one, "grp", scatter_dimension=0, tiled=True)
    gain_local = jnp.sum(d_normed * wide_tokens * inv_rms, axis=0)
    gain_total = lax.psum(gain_local, ("rep", "grp"))
    scaled = d_normed * norm_gain
    inner_mean = jnp.mean(scaled * wide_tokens, axis=1, keepdims=True)
    token_grad = (inv_rms * (scaled - wide_tokens * inv_rms * inv_rms * inner_mean)).astype(
        jnp.bfloat16
    )
    return (token_grad, weight_sum * grad_scale, gain_total * grad_scale)


def shards(tokens, norm_gain, key_weight, key_grad):
    n_rep, n_grp = lax.axis_size("rep"), lax.axis_size("grp")
    n_z = n_grp // 2
    if (
        n_rep == 2 * 2 and n_grp == 2 * 4
        and key_weight.shape[1] % (n_rep * LANES) == 0 and key_weight.shape[0] % 16 == 0
        and tokens.shape[1] % (2 * LANES) == 0 and tokens.shape[0] % LANES == 0
    ):
        return fused(n_rep, n_grp, tokens, norm_gain, key_weight, key_grad)
    return plain(tokens, norm_gain, key_weight, key_grad)


def solution(mesh):
    in_specs = (P(("rep", "grp"), None), P(), P("grp", None), P(("rep", "grp"), None))
    out_specs = (P(("rep", "grp"), None), P("grp", "rep"), P())
    return jax.shard_map(shards, mesh=mesh, in_specs=in_specs, out_specs=out_specs, check_vma=False)
```
